32 devices in a mesh: gx: 8 (over z, x), gy: 4 (over y, core).
Axes of the slice: x: 2, y: 2, z: 4, core: 2. Of those that a mesh axis runs over, the one named last changes fastest.
Arguments:
- pooled: bfloat16 [4096, 8, 128], P(('gx', 'gy')), may hold values from -6 to 6
- cotangent: bfloat16 [4096, 28, 128], P(('gx', 'gy')), may hold values from -0.09375 to 0.09375
- bilinear: bfloat16 [7, 128, 128], replicated, may hold values from -0.5 to 0.5
- bag_ids: int32 [4096, 8, 4], P(('gx', 'gy')), may hold values from 0 to 8191, as said below
- bag_lens: int32 [4096, 8], P(('gx', 'gy')), may hold values from 1 to 4
- row_home: int32 [8, 8192], replicated, may hold values from 0 to 8191, as said below
Outputs:
- weight_grad: float32 [7, 128, 128], replicated
- table_grad: float32 [8192, 8, 128], P(('gx', 'gy'))
The draws below stay inside these ranges and needn't reach their ends.
Inputs may be any that keep to these rules, and one draw needn't show every extreme that they name: Each row row_home[f] is a permutation; row r of field f's table is stored at position row_home[f, r] of table_grad's first dimension. Only the first bag_lens entries of a bag are live. The stored position q = row_home[f, bag_ids[sample, f, k]] of an entry lies in the block of 256 positions of device q // 256 (devices in gx+gy order); among all entries of one device's samples, live or not, at most 256 lie in any one device's block; in every device's entries some block is hit exactly 256 times, and one block is hit exactly 256 times by the entries of every device.
All inputs are finite; a program needn't handle non-finite values.
Results may differ from the reference program's by a relative error of at most 0.0035.
Values may be sent and summed in bfloat16 or wider, within the bound.
No kernel may reach another device: no remote copies, remote signals or barrier semaphores. Data moves between devices by JAX's collectives and lax.ppermute only.
A program may use at most 64 MiB of HBM per device.

```python
import jax
import jax.numpy as jnp
from jax import lax

D = 128
FIELDS = 8
PAIRS = 28
BAG = 4
TOK_DEV = 128
R_DEV = 256
TOKENS = 4096
ROWS = 8192
CAP = 256
N_GX = 8
N_GY = 4


def home_table(key):
    field_keys = jax.random.split(jax.random.fold_in(key, 101), FIELDS)
    return jax.vmap(lambda k: jax.random.permutation(k, ROWS))(field_keys).astype(jnp.int32)


def draw_row_home(key, part):
    return home_table(key)


def draw_bag_ids(key, part):
    home = home_table(key)
    inverse = jnp.argsort(home, axis=1, stable=True).astype(jnp.int32)
    owners_all = N_GX * N_GY
    slots = CAP * owners_all
    entries = TOK_DEV * FIELDS * BAG
    route_key = jax.random.fold_in(key, 202)
    hotness = jax.random.randint(jax.random.fold_in(route_key, 1), (owners_all,), 0, 4).astype(jnp.int32)
    shared_full = jax.random.randint(jax.random.fold_in(route_key, 2), (), 0, owners_all).astype(jnp.int32)
    slot_owner = (jnp.arange(slots, dtype=jnp.int32) // CAP).astype(jnp.int32)

    def one_block(block):
        block_key = jax.random.fold_in(route_key, 1000 + block)
        raw = jax.random.randint(jax.random.fold_in(block_key, 1), (slots,), 0, 4096).astype(jnp.int32)
        score = jnp.right_shift(raw, 2 * hotness[slot_owner])
        own_full = jax.random.randint(jax.random.fold_in(block_key, 2), (), 0, owners_all).astype(jnp.int32)
        forced = jnp.logical_or(slot_owner == own_full, slot_owner == shared_full)
        score = jnp.where(forced, -1, score)
        rank_key = score * slots + jnp.arange(slots, dtype=jnp.int32)
        picked = jnp.argsort(rank_key, stable=True)[:entries]
        owners = slot_owner[picked]
        owners = owners[jax.random.permutation(jax.random.fold_in(block_key, 3), entries)]
        first = jax.random.randint(jax.random.fold_in(block_key, 4), (entries,), 0, R_DEV).astype(jnp.int32)
        second = jax.random.randint(jax.random.fold_in(block_key, 5), (entries,), 0, R_DEV).astype(jnp.int32)
        local = first * second // R_DEV
        return (owners * R_DEV + local).astype(jnp.int32)
    stored = lax.map(one_block, jnp.arange(owners_all, dtype=jnp.int32)).reshape(TOKENS, FIELDS, BAG)
    field_index = jnp.arange(FIELDS, dtype=jnp.int32)[None, :, None]
    return inverse[field_index, stored].astype(jnp.int32)


def plant(result, key, low, high):
    spot = [jax.random.randint(jax.random.fold_in(key, axis), (), 0, length) for axis, length in enumerate(result.shape)]
    widest = result.shape.index(max(result.shape))
    beside = spot[:widest] + [(spot[widest] + 1) % result.shape[widest]] + spot[widest + 1:]
    return result.at[tuple(spot)].set(low).at[tuple(beside)].set(high)


def steps_of(stream_key, extent, cuts, smallest, largest):
    gain = 1.0
    for axis_at, blocks in cuts:
        draws = jax.random.uniform(jax.random.fold_in(jax.random.fold_in(stream_key, 6), axis_at), (blocks,), jnp.float32, smallest / len(cuts), largest / len(cuts))
        gain = gain * jnp.repeat(jnp.exp(draws), extent[axis_at] // blocks).reshape((-1,) + (1,) * (len(extent) - 1 - axis_at))
    return gain


def scatter_about(key, shape, width, most, shards=(), held_as=jnp.bfloat16):
    level = steps_of(key, shape, shards, -0.22, 0.18) if shards else 1.0
    result = jax.random.normal(key, shape, jnp.float32) * width * level
    return jnp.minimum(jnp.maximum(result, -most), most).astype(held_as)


def setup_inputs(seed: int = 0) -> dict:
    key_of = jax.random.split(jax.random.key(seed), 7)
    return {
        "pooled": scatter_about(key_of[0], (TOKENS, FIELDS, D), 1.0, 6.0, ((0, 32),)),
        "cotangent": scatter_about(key_of[1], (TOKENS, PAIRS, D), TOKENS ** -0.5, 0.09375, ((0, 32),)),
        "bilinear": scatter_about(key_of[2], (FIELDS - 1, D, D), D ** -0.5, 0.5),
        "bag_ids": draw_bag_ids(jax.random.fold_in(key_of[6], 71), 0),
        "bag_lens": plant(jax.random.randint(key_of[4], (TOKENS, FIELDS), 1, BAG + 1), jax.random.fold_in(key_of[4], 1), 1, BAG).astype(jnp.int32),
        "row_home": draw_row_home(jax.random.fold_in(key_of[6], 71), 0),
    }


def pair_list(fields):
    return [(i, j) for i in range(fields) for j in range(i + 1, fields)]


def reference(pooled, cotangent, bilinear, bag_ids, bag_lens, row_home):
    pair_order = pair_list(FIELDS)
    embedded = pooled.astype(jnp.float32)
    weights = bilinear.astype(jnp.float32)
    cot_rows = cotangent.astype(jnp.float32)
    projected = jnp.einsum('bfd,fde->bfe', embedded[:, :FIELDS - 1], weights)
    upper_terms = []
    for i in range(FIELDS - 1):
        running = jnp.zeros((TOKENS, D), jnp.float32)
        for p, (a, c) in enumerate(pair_order):
            if a == i:
                running = running + cot_rows[:, p] * embedded[:, c]
        upper_terms.append(running)
    upper_bf = jnp.stack(upper_terms, 1).astype(jnp.bfloat16).astype(jnp.float32)
    weight_grad = jnp.einsum('bfd,bfe->fde', embedded[:, :FIELDS - 1], upper_bf)
    field_list = []
    for i in range(FIELDS):
        running = jnp.zeros((TOKENS, D), jnp.float32)
        if i < FIELDS - 1:
            running = running + jnp.einsum('be,de->bd', upper_bf[:, i], weights[i])
        for p, (a, c) in enumerate(pair_order):
            if c == i:
                running = running + cot_rows[:, p] * projected[:, a]
        field_list.append(running)
    field_grads = jnp.stack(field_list, 1).astype(jnp.bfloat16).astype(jnp.float32)
    live = jnp.arange(BAG, dtype=jnp.int32)[None, :]
    tables = []
    for f in range(FIELDS):
        stored = row_home[f][bag_ids[:, f, :]]
        segment = jnp.where(live < bag_lens[:, f, None], stored, ROWS).astype(jnp.int32)
        values = jnp.broadcast_to(field_grads[:, f, None, :], (TOKENS, BAG, D)).reshape(TOKENS * BAG, D)
        summed = jax.ops.segment_sum(values, segment.reshape(-1), num_segments=ROWS + 1)
        tables.append(summed[:ROWS])
    return weight_grad, jnp.stack(tables, 1)
```

```python
import functools

import jax
import jax.numpy as jnp
from jax import lax
from jax.experimental import pallas as pl
from jax.experimental.pallas import tpu as pltpu
from jax.sharding import PartitionSpec as P


AXES = ("gx", "gy")
CHUNKS = 2
F32, BF16, I32 = jnp.float32, jnp.bfloat16, jnp.int32
VMEM = pl.BlockSpec(memory_space=pltpu.VMEM)
SMEM = pl.BlockSpec(memory_space=pltpu.SMEM)


def dot(a, b, ca, cb):
    return lax.dot_general(a, b, (((ca,), (cb,)), ((), ())), preferred_element_type=F32)


def pair_index(fields):
    order = [(i, j) for i in range(fields) for j in range(i + 1, fields)]
    return {pair: p for p, pair in enumerate(order)}


def local_kernel(dims, place, pooled, cot, bil, ids, lens, home, *rest):
    fields, samples, bag, r_dev, chunks = dims
    grads, (meta, weight_keep, weight_send) = rest[:chunks], rest[chunks : chunks + 3]
    flat, table, codes, weight = rest[chunks + 3 :]
    width = 128
    per_chunk = fields // chunks
    pairs = pair_index(fields)

    flat[...] = pooled[...].reshape(samples * fields, width).astype(F32)
    emb = [flat[pl.ds(f, samples, stride=fields), :] for f in range(fields)]
    emb_bf = [e.astype(BF16) for e in emb]

    rows = home.shape[1]
    leads = rows // width
    for h in range(leads):
        table[pl.ds(h, fields, stride=leads), :] = home[:, h * width : (h + 1) * width]
    entries = bag * samples
    lead_iota = lax.broadcasted_iota(I32, (leads, entries), 0)
    lane_iota = lax.broadcasted_iota(I32, (width, entries), 0)
    for f in range(fields):
        id_row = jnp.concatenate([ids[f * bag + k : f * bag + k + 1, :] for k in range(bag)], 1)
        lead = id_row // width
        lane = id_row - lead * width
        chosen = (lead_iota == lead).astype(F32).astype(BF16)
        tab = table[f * leads : (f + 1) * leads, :]
        tab_owner = tab // r_dev
        tab_local = tab - tab_owner * r_dev
        both = jnp.concatenate([tab_owner.astype(F32), tab_local.astype(F32)], 1).astype(BF16)
        picked = dot(both, chosen, 0, 0)
        hit = lane_iota == lane
        owner = jnp.sum(jnp.where(hit, picked[:width], 0.0), axis=0, keepdims=True)
        local = jnp.sum(jnp.where(hit, picked[width:], 0.0), axis=0, keepdims=True)
        for k in range(bag):
            part = slice(k * samples, (k + 1) * samples)
            alive = lens[f : f + 1, :] > k
            codes[f * bag + k : f * bag + k + 1, :] = jnp.where(alive, owner[:, part], -1.0)
            at = (fields + f) * bag + k
            codes[at : at + 1, :] = local[:, part]
    owners = [codes[pl.ds(k, fields, stride=bag), :] for k in range(bag)]
    locals_ = [codes[pl.ds(fields * bag + k, fields, stride=bag), :] for k in range(bag)]
    for k in range(bag):
        count = jnp.ones((fields, samples), F32)
        mine = owners[k]
        for m in range(bag):
            if m != k:
                same = jnp.logical_and(owners[k] == owners[m], locals_[k] == locals_[m])
                if m > k:
                    count = count + jnp.where(same, 1.0, 0.0)
                else:
                    mine = jnp.where(same, -1.0, mine)
        codes[pl.ds(k, fields, stride=bag), :] = mine
        codes[pl.ds(2 * fields * bag + k, fields, stride=bag), :] = count
    meta[...] = codes[...].astype(BF16)

    projected = [dot(emb_bf[i], bil[i], 1, 0) for i in range(fields - 1)]
    for f in range(fields):
        total = jnp.zeros((samples, width), F32)
        if f < fields - 1:
            upper = jnp.zeros((samples, width), F32)
            for j in range(f + 1, fields):
                upper = upper + cot[pairs[(f, j)]].astype(F32) * emb[j]
            upper = upper.astype(BF16)
            weight[f * width : (f + 1) * width, :] = dot(emb_bf[f], upper, 0, 0)
            total = dot(upper, bil[f], 1, 1)
        for k in range(f):
            total = total + cot[pairs[(k, f)]].astype(F32) * projected[k]
        at = f % per_chunk * samples
        grads[f // per_chunk][at : at + samples, :] = total.astype(BF16)
    half = weight_keep.shape[0]
    core = place[0]
    weight_keep[...] = weight[pl.ds(pl.multiple_of(core * half, 8), half), :]
    weight_send[...] = weight[pl.ds(pl.multiple_of((1 - core) * half, 8), half), :]


def split_kernel(depth, place, keep, got, *outs):
    total = outs[-1]
    total[...] = keep[...] + got[...]
    rows = outs[0].shape[0]
    z = place[1]
    for d in range(depth):
        target = lax.rem(z + d, depth)
        outs[d][...] = total[pl.ds(pl.multiple_of(target * rows, 8), rows), :]


def plane_kernel(dims, owner_ids, *refs):
    fields, bag, senders, owners, first, count_fields, samples, r_dev = dims
    metas, grads = refs[:senders], refs[senders : 2 * senders]
    outs = refs[2 * senders : 2 * senders + owners]
    want, times, counts = refs[2 * senders + owners :]
    rows = fields * bag
    for s in range(senders):
        code = metas[s][...].astype(F32)
        times[s] = code[2 * rows :]
        for o in range(owners):
            match = code[:rows] == owner_ids[o].astype(F32)
            want[o * senders + s] = jnp.where(match, code[rows : 2 * rows], -1.0)
    tile = 16
    base = lax.broadcasted_iota(I32, (tile, samples), 0).astype(F32)
    iotas = [(base + float(j * tile)).astype(BF16) for j in range(r_dev // tile)]
    for o in range(owners):

        def field(f, _, o=o):
            at = (first + f) * bag
            for s in range(senders):
                pos, num = [], []
                for k in range(bag):
                    row = want[o * senders + s, pl.ds(at + k, 1), :]
                    pos.append(jnp.broadcast_to(row, (tile, samples)).astype(BF16))
                    row = times[s, pl.ds(at + k, 1), :]
                    num.append(jnp.broadcast_to(row, (tile, samples)).astype(BF16))
                for j in range(r_dev // tile):
                    piece = jnp.zeros((tile, samples), BF16)
                    for k in range(bag):
                        piece = jnp.where(pos[k] == iotas[j], num[k], piece)
                    counts[s, j * tile : (j + 1) * tile, :] = piece
            left = jnp.concatenate([counts[s] for s in range(senders)], 1)
            here = pl.ds(pl.multiple_of(f * samples, samples), samples)
            right = jnp.concatenate([grads[s][here, :] for s in range(senders)], 0)
            there = pl.ds(pl.multiple_of(f * r_dev, r_dev), r_dev)
            outs[o][there, :] = dot(left, right, 1, 0).astype(outs[o].dtype)
            return 0

        lax.fori_loop(0, count_fields, field, 0)


def finish_kernel(dims, place, *refs):
    fields, chunks, owners, depth, r_dev = dims
    refs = list(refs)
    parts = [[refs.pop(0) for _ in range(owners)] for _ in range(chunks)]
    table_out = refs[-1]
    per_chunk = fields // chunks
    for c in range(chunks):
        for f in range(per_chunk):
            part = slice(f * r_dev, (f + 1) * r_dev)
            total = parts[c][0][part, :]
            for o in range(1, owners):
                total = total + parts[c][o][part, :].astype(F32)
            table_out[pl.ds(c * per_chunk + f, r_dev, stride=fields), :] = total


def gather_kernel(depth, place, *refs):
    out = refs[-1]
    rows = refs[0].shape[0]
    z = place[1]
    for d in range(depth):
        source = lax.rem(z - d + depth, depth)
        out[pl.ds(pl.multiple_of(source * rows, 8), rows), :] = refs[d][...]


def halves_kernel(place, mine, other, out):
    half = mine.shape[0]
    core = place[0]
    out[pl.ds(pl.multiple_of(core * half, 8), half), :] = mine[...]
    out[pl.ds(pl.multiple_of((1 - core) * half, 8), half), :] = other[...]


def tree_sum(terms):
    while len(terms) > 1:
        terms = [terms[i] + terms[i + 1] for i in range(0, len(terms), 2)]
    return terms[0]


def call(kernel, outs, args, scratch=(), flops=0, scalars=1):
    size = sum(a.size * a.dtype.itemsize for a in args)
    return pl.pallas_call(
        kernel,
        out_shape=outs,
        in_specs=[SMEM] * scalars + [VMEM] * (len(args) - scalars),
        out_specs=[VMEM] * len(outs),
        scratch_shapes=list(scratch),
        cost_estimate=pl.CostEstimate(flops=flops, bytes_accessed=size, transcendentals=0),
    )(*args)


def on_device(pooled, cotangent, bilinear, bag_ids, bag_lens, row_home):
    samples, fields, width = pooled.shape
    bag = bag_ids.shape[2]
    gx, gy = lax.axis_size("gx"), lax.axis_size("gy")
    devices = gx * gy
    depth, plane = gx // 2, 2 * gy
    r_dev = row_home.shape[1] // devices
    me = lax.axis_index(AXES)
    core, z = me % 2, me // plane
    place = jnp.stack([core, z]).astype(I32)
    columns = plane // 2
    owner_ids = jnp.stack([me ^ (2 * m) for m in range(columns)]).astype(I32)

    def shift_z(a, d):
        perm = [(s, (s + d * plane) % devices) for s in range(devices)]
        return lax.ppermute(a, AXES, perm)

    def flip(a, m):
        return lax.ppermute(a, AXES, [(s, s ^ m) for s in range(devices)])

    f32 = lambda *s: jax.ShapeDtypeStruct(s, F32)
    bf16 = lambda *s: jax.ShapeDtypeStruct(s, BF16)
    chunks, per_chunk = CHUNKS, fields // CHUNKS
    w_rows = (fields - 1) * width
    rows = fields * bag
    leads = row_home.shape[1] // width
    out = call(
        functools.partial(local_kernel, (fields, samples, bag, r_dev, chunks)),
        [bf16(per_chunk * samples, width)] * chunks
        + [bf16(3 * rows, samples), f32(w_rows // 2, width), f32(w_rows // 2, width)],
        [
            place,
            pooled,
            cotangent.transpose(1, 0, 2),
            bilinear,
            bag_ids.transpose(1, 2, 0).reshape(rows, samples),
            bag_lens.T,
            row_home,
        ],
        [
            pltpu.VMEM((samples * fields, width), F32),
            pltpu.VMEM((fields * leads, width), I32),
            pltpu.VMEM((3 * rows, samples), F32),
            pltpu.VMEM((w_rows, width), F32),
        ],
        flops=30_000_000,
    )
    grads, (meta, w_keep, w_send) = out[:chunks], out[chunks:]

    def everywhere(a):
        column = [a] + [shift_z(a, d) for d in range(1, depth)]
        return column + [flip(b, 1) for b in column]

    metas = everywhere(meta)
    senders = 2 * depth
    parts = []
    for c in range(chunks):
        blocks = everywhere(grads[c])
        sums = call(
            functools.partial(
                plane_kernel,
                (fields, bag, senders, columns, c * per_chunk, per_chunk, samples, r_dev),
            ),
            [f32(per_chunk * r_dev, width)] + [bf16(per_chunk * r_dev, width)] * (columns - 1),
            [owner_ids] + metas + blocks,
            [
                pltpu.VMEM((columns * senders, rows, samples), F32),
                pltpu.VMEM((senders, rows, samples), F32),
                pltpu.VMEM((senders, r_dev, samples), BF16),
            ],
            flops=2_000_000_000 // chunks,
        )
        parts.append([sums[0]] + [flip(sums[m], 2 * m) for m in range(1, columns)])

    shares = call(
        functools.partial(split_kernel, depth),
        [f32(w_rows // 2 // depth, width)] * depth,
        [place, w_keep, flip(w_send, 1)],
        [pltpu.VMEM((w_rows // 2, width), F32)],
    )
    share = shares[0]
    for d in range(1, depth):
        share = share + shift_z(shares[d], d)
    share = tree_sum([share] + [flip(share, 2 * m) for m in range(1, columns)])
    half = call(
        functools.partial(gather_kernel, depth),
        [f32(w_rows // 2, width)],
        [place, share] + [shift_z(share, d) for d in range(1, depth)],
    )[0]
    weight_grad = call(halves_kernel, [f32(w_rows, width)], [place, half, flip(half, 1)])[0]

    table = call(
        functools.partial(finish_kernel, (fields, chunks, columns, depth, r_dev)),
        [f32(r_dev * fields, width)],
        [place] + sum(parts, []),
    )[0]
    return weight_grad.reshape(fields - 1, width, width), table.reshape(r_dev, fields, width)


def solution(mesh):
    placed = (
        P(AXES, None, None),
        P(AXES, None, None),
        P(),
        P(AXES, None, None),
        P(AXES, None),
        P(),
    )
    return jax.shard_map(
        on_device,
        mesh=mesh,
        in_specs=placed,
        out_specs=(P(), P(AXES, None, None)),
        check_vma=False,
    )
```

```python
import functools

import jax
import jax.numpy as jnp
from jax import lax
from jax.experimental import pallas as pl
from jax.experimental.pallas import tpu as pltpu
from jax.sharding import PartitionSpec as P


AXES = ("gx", "gy")
CHUNKS = 2
WIDTH = 128
F32, BF16, I32 = jnp.float32, jnp.bfloat16, jnp.int32
VMEM = pl.BlockSpec(memory_space=pltpu.VMEM)


def dot(a, b, ca, cb):
    return lax.dot_general(a, b, (((ca,), (cb,)), ((), ())), preferred_element_type=F32)


def my_place(depth, plane):
    me = lax.axis_index("gx") * lax.axis_size("gy") + lax.axis_index("gy")
    return lax.rem(me, plane), lax.div(me, plane)


def pair_index(fields):
    order = [(i, j) for i in range(fields) for j in range(i + 1, fields)]
    return {pair: p for p, pair in enumerate(order)}


def write_codes(cfg, group, ids, lens, home, table, codes):
    fields, samples, bag, r_dev = cfg
    rows = home.shape[1]
    leads = rows // WIDTH
    entries = bag * samples
    n = len(group)
    for h in range(leads):
        table[pl.ds(h, fields, stride=leads), :] = home[:, h * WIDTH : (h + 1) * WIDTH]
    lead_iota = lax.broadcasted_iota(I32, (leads, entries), 0)
    lane_iota = lax.broadcasted_iota(I32, (WIDTH, entries), 0)
    for i, f in enumerate(group):
        id_row = jnp.concatenate([ids[f * bag + k : f * bag + k + 1, :] for k in range(bag)], 1)
        lead = id_row // WIDTH
        lane = id_row - lead * WIDTH
        chosen = (lead_iota == lead).astype(F32).astype(BF16)
        tab = table[f * leads : (f + 1) * leads, :]
        tab_owner = tab // r_dev
        tab_local = tab - tab_owner * r_dev
        both = jnp.concatenate([tab_owner.astype(F32), tab_local.astype(F32)], 1).astype(BF16)
        picked = dot(both, chosen, 0, 0)
        hit = lane_iota == lane
        owner = jnp.sum(jnp.where(hit, picked[:WIDTH], 0.0), axis=0, keepdims=True)
        local = jnp.sum(jnp.where(hit, picked[WIDTH:], 0.0), axis=0, keepdims=True)
        owners, locals_ = [], []
        for k in range(bag):
            part = slice(k * samples, (k + 1) * samples)
            alive = lens[f : f + 1, :] > k
            owners.append(jnp.where(alive, owner[:, part], -1.0))
            locals_.append(local[:, part])
        for k in range(bag):
            count = jnp.ones((1, samples), F32)
            mine = owners[k]
            for m in range(bag):
                if m != k:
                    same = jnp.logical_and(owners[k] == owners[m], locals_[k] == locals_[m])
                    if m > k:
                        count = count + jnp.where(same, 1.0, 0.0)
                    else:
                        mine = jnp.where(same, -1.0, mine)
            codes[i * bag + k : i * bag + k + 1, :] = mine
            codes[(n + i) * bag + k : (n + i) * bag + k + 1, :] = locals_[k]
            codes[(2 * n + i) * bag + k : (2 * n + i) * bag + k + 1, :] = count


def local_kernel(cfg, groups, w_from, plane, depth, *refs):
    fields, samples, bag, r_dev = cfg
    pooled, cot, bil, ids, lens, home = refs[:6]
    refs = refs[6:]
    last = w_from is not None
    if last:
        w_before, refs = refs[0], refs[1:]
    messages, refs = refs[: len(groups)], refs[len(groups) :]
    flat, table, codes = refs[-3:]
    pairs = pair_index(fields)

    flat[...] = pooled[...].reshape(samples * fields, WIDTH).astype(F32)
    emb = [flat[pl.ds(f, samples, stride=fields), :] for f in range(fields)]
    emb_bf = [e.astype(BF16) for e in emb]
    top = max(max(g) for g in groups)
    projected = [dot(emb_bf[i], bil[i], 1, 0) for i in range(min(top, fields - 1))]
    weight = refs[-4] if last else refs[0]
    for message, group in zip(messages, groups):
        for i, f in enumerate(group):
            total = jnp.zeros((samples, WIDTH), F32)
            if f < fields - 1:
                upper = jnp.zeros((samples, WIDTH), F32)
                for j in range(f + 1, fields):
                    upper = upper + cot[pairs[(f, j)]].astype(F32) * emb[j]
                upper = upper.astype(BF16)
                weight[f * WIDTH : (f + 1) * WIDTH, :] = dot(emb_bf[f], upper, 0, 0)
                total = dot(upper, bil[f], 1, 1)
            for k in range(f):
                total = total + cot[pairs[(k, f)]].astype(F32) * projected[k]
            message[i * samples : (i + 1) * samples, :] = total.astype(BF16)
        write_codes(cfg, group, ids, lens, home, table, codes)
        message[len(group) * samples :, :] = codes[...].astype(BF16)
    if last:
        weight[:w_from, :] = w_before[...]
        full = weight.shape[0]
        if full > (fields - 1) * WIDTH:
            used = (fields - 1) * WIDTH
            weight[used:, :] = jnp.zeros((full - used, WIDTH), F32)
        shares = refs[:plane]
        rows = full // plane
        p, _ = my_place(depth, plane)
        for m in range(plane):
            at = pl.multiple_of((p ^ m) * rows, 8)
            shares[m][...] = weight[pl.ds(at, rows), :]


def plane_kernel(cfg, n, senders, columns, plane, depth, mode, *refs):
    fields, samples, bag, r_dev = cfg
    refs = list(refs)
    blocks = [refs.pop(0) for _ in range(senders)]
    extra = [refs.pop(0) for _ in range({"": 0, "plane": plane, "depth": depth}[mode])]
    outs = [refs.pop(0) for _ in range(columns)]
    share = refs.pop(0) if mode else None
    want, times, order = refs
    rows = n * bag
    p, z = my_place(depth, plane)
    if mode == "plane":
        total = extra[0][...]
        for e in extra[1:]:
            total = total + e[...]
        share[...] = total
    if mode == "depth":
        for d in range(depth):
            order[lax.rem(z - d + depth, depth)] = extra[d][...]
        total = order[0]
        for d in range(1, depth):
            total = total + order[d]
        share[...] = total
    for s in range(senders):
        code = blocks[s][n * samples :, :].astype(F32)
        times[s] = code[2 * rows :]
        for o in range(columns):
            owner = (z * plane + (p ^ (2 * o))).astype(F32)
            want[o * senders + s] = jnp.where(code[:rows] == owner, code[rows : 2 * rows], -1.0)
    tile = 16
    base = lax.broadcasted_iota(I32, (tile, samples), 0).astype(F32)
    iotas = [(base + float(j * tile)).astype(BF16) for j in range(r_dev // tile)]
    for o in range(columns):

        def field(f, _, o=o):
            total = None
            here = pl.ds(pl.multiple_of(f * samples, samples), samples)
            for first in range(0, senders, 2):
                lefts = []
                for s in (first, first + 1):
                    pos, num = [], []
                    for k in range(bag):
                        row = want[o * senders + s, pl.ds(f * bag + k, 1), :]
                        pos.append(jnp.broadcast_to(row, (tile, samples)).astype(BF16))
                        row = times[s, pl.ds(f * bag + k, 1), :]
                        num.append(jnp.broadcast_to(row, (tile, samples)).astype(BF16))
                    pieces = []
                    for iota in iotas:
                        piece = jnp.zeros((tile, samples), BF16)
                        for k in range(bag):
                            piece = jnp.where(pos[k] == iota, num[k], piece)
                        pieces.append(piece)
                    lefts.append(jnp.concatenate(pieces, 0))
                left = jnp.concatenate(lefts, 1)
                right = jnp.concatenate([blocks[first][here, :], blocks[first + 1][here, :]], 0)
                part = dot(left, right, 1, 0)
                total = part if total is None else total + part
            there = pl.ds(pl.multiple_of(f * r_dev, r_dev), r_dev)
            outs[o][there, :] = total.astype(outs[o].dtype)
            return 0

        lax.fori_loop(0, n, field, 0)


def finish_kernel(cfg, chunks, columns, plane, depth, *refs):
    fields, samples, bag, r_dev = cfg
    refs = list(refs)
    shares = [refs.pop(0) for _ in range(plane)]
    parts = [[refs.pop(0) for _ in range(columns)] for _ in range(chunks)]
    weight_out, table_out, weight = refs
    p, _ = my_place(depth, plane)
    rows = shares[0].shape[0]
    for m in range(plane):
        weight[pl.ds(pl.multiple_of((p ^ m) * rows, 8), rows), :] = shares[m][...]
    weight_out[...] = weight[: weight_out.shape[0], :]
    n = fields // chunks
    for c in range(chunks):
        for f in range(n):
            part = slice(f * r_dev, (f + 1) * r_dev)
            total = parts[c][0][part, :]
            for o in range(1, columns):
                total = total + parts[c][o][part, :].astype(F32)
            table_out[pl.ds(c * n + f, r_dev, stride=fields), :] = total


def call(kernel, outs, args, scratch=(), flops=0):
    size = sum(a.size * a.dtype.itemsize for a in args)
    return pl.pallas_call(
        kernel,
        out_shape=outs,
        in_specs=[VMEM] * len(args),
        out_specs=[VMEM] * len(outs),
        scratch_shapes=[pltpu.VMEM(*s) for s in scratch],
        cost_estimate=pl.CostEstimate(flops=flops, bytes_accessed=size, transcendentals=0),
        compiler_params=pltpu.CompilerParams(vmem_limit_bytes=24 * 2**20),
    )(*args)


def on_device(pooled, cotangent, bilinear, bag_ids, bag_lens, row_home):
    samples, fields, _ = pooled.shape
    bag = bag_ids.shape[2]
    gx, gy = lax.axis_size("gx"), lax.axis_size("gy")
    devices = gx * gy
    depth, plane = gx // 2, 2 * gy
    columns, senders = plane // 2, 2 * depth
    r_dev = row_home.shape[1] // devices
    cfg = (fields, samples, bag, r_dev)

    def shift_z(a, d):
        perm = [(s, (s + d * plane) % devices) for s in range(devices)]
        return lax.ppermute(a, AXES, perm)

    def flip(a, m):
        return lax.ppermute(a, AXES, [(s, s ^ m) for s in range(devices)])

    def f32(*s):
        return jax.ShapeDtypeStruct(s, F32)

    def bf16(*s):
        return jax.ShapeDtypeStruct(s, BF16)

    chunks, n = CHUNKS, fields // CHUNKS
    groups = [list(range(c * n, (c + 1) * n)) for c in range(chunks)]
    leads = row_home.shape[1] // WIDTH
    w_first = min(n, fields - 1) * WIDTH
    share = -(-(fields - 1) * WIDTH // (8 * plane)) * 8
    inputs = [
        pooled,
        cotangent.transpose(1, 0, 2),
        bilinear,
        bag_ids.transpose(1, 2, 0).reshape(fields * bag, samples),
        bag_lens.T,
        row_home,
    ]
    message = bf16(n * samples + 3 * n * bag, WIDTH)
    scratch = [
        ((samples * fields, WIDTH), F32),
        ((fields * leads, WIDTH), I32),
        ((3 * n * bag, samples), F32),
    ]
    first, w_before = call(
        functools.partial(local_kernel, cfg, groups[:1], None, plane, depth),
        [message, f32(w_first, WIDTH)],
        inputs,
        scratch,
        flops=15_000_000,
    )
    rest = call(
        functools.partial(local_kernel, cfg, groups[1:], w_first, plane, depth),
        [message] * (chunks - 1) + [f32(share, WIDTH)] * plane,
        inputs + [w_before],
        [((share * plane, WIDTH), F32)] + scratch,
        flops=15_000_000,
    )
    messages = [first] + list(rest[: chunks - 1])
    shares = list(rest[chunks - 1 :])
    shares = [shares[0]] + [flip(shares[m], m) for m in range(1, plane)]
    modes = {0: ("plane", lambda: shares), chunks - 1: ("depth", lambda: column)}
    parts = []
    for c in range(chunks):
        blocks = [messages[c]] + [shift_z(messages[c], d) for d in range(1, depth)]
        blocks = blocks + [flip(b, 1) for b in blocks]
        mode, extra = modes.get(c, ("", lambda: []))
        sums = call(
            functools.partial(plane_kernel, cfg, n, senders, columns, plane, depth, mode),
            [f32(n * r_dev, WIDTH)]
            + [bf16(n * r_dev, WIDTH)] * (columns - 1)
            + ([f32(share, WIDTH)] if mode else []),
            blocks + extra(),
            [
                ((columns * senders, n * bag, samples), F32),
                ((senders, n * bag, samples), F32),
                ((depth, share, WIDTH), F32),
            ],
            flops=2_000_000_000 // chunks,
        )
        parts.append([sums[0]] + [flip(sums[m], 2 * m) for m in range(1, columns)])
        if mode == "plane":
            column = [sums[-1]] + [shift_z(sums[-1], d) for d in range(1, depth)]
        if mode == "depth":
            mine = [sums[-1]] + [flip(sums[-1], 2 * m) for m in range(1, columns)]
    finals = [a for b in mine for a in (b, flip(b, 1))]
    weight_grad, table = call(
        functools.partial(finish_kernel, cfg, chunks, columns, plane, depth),
        [f32((fields - 1) * WIDTH, WIDTH), f32(r_dev * fields, WIDTH)],
        finals + sum(parts, []),
        [((share * plane, WIDTH), F32)],
        flops=1_000_000,
    )
    return weight_grad.reshape(fields - 1, WIDTH, WIDTH), table.reshape(r_dev, fields, WIDTH)


def solution(mesh):
    placed = (
        P(AXES, None, None),
        P(AXES, None, None),
        P(),
        P(AXES, None, None),
        P(AXES, None),
        P(),
    )
    return jax.shard_map(
        on_device,
        mesh=mesh,
        in_specs=placed,
        out_specs=(P(), P(AXES, None, None)),
        check_vma=False,
    )
```
